32 devices in a mesh: gene: 8 (over z, x), cell: 4 (over y, core).
Axes of the slice: x: 2, y: 2, z: 4, core: 2. Of those that a mesh axis runs over, the one named last changes fastest.
Arguments:
- pool_counts: bfloat16 [20480, 16384], P('gene', 'cell'), may hold values from 0 to 6.5
- cell_picks: int32 [7, 4096], P(None, 'cell'), may hold values from 0 to 16383, as said below
- loadings_init: float32 [64, 20480], P(None, 'gene'), may hold values from -0.0390625 to 0.0390625
Outputs:
- scaled_loadings: float32 [64, 20480], P(None, 'gene')
The draws below stay inside these ranges and needn't reach their ends.
Inputs may be any that keep to these rules, and one draw needn't show every extreme that they name: `cell_picks`: column b of every row names a pool cell in [(b // 1024) * 4096, (b // 1024 + 1) * 4096); no cell is named twice in one row.
All inputs are finite; a program needn't handle non-finite values.
Results may differ from the reference program's by a relative error of at most 0.018.
Values may be sent and summed in bfloat16 or wider, within the bound.
A program may use at most 128 MiB of HBM per device.

```python
import math
import jax
import jax.numpy as jnp
from jax import lax

GENES = 20480
COMPS = 64
STEPS = 7
BATCH_DEV = 1024
POOL_DEV = 4096
BATCH = 4096
POOL = 16384


def draw_pool_counts(key, part):
    scale_key, noise_key = jax.random.split(jax.random.fold_in(key, 11))
    genes = jnp.arange(GENES, dtype=jnp.float32)
    rising = 1.0 + 2.0 * genes / max(GENES - 1, 1)
    lowest, highest = (math.log(0.1), math.log(10.0))
    gene_scale = jnp.exp(jax.random.uniform(scale_key, (GENES,), jnp.float32, lowest, highest)) * rising
    noise = jnp.minimum(jax.random.exponential(noise_key, (GENES, POOL), jnp.float32), 12.0)
    return jnp.log1p(gene_scale[:, None] * noise).astype(jnp.bfloat16)


def draw_cell_picks(key, part):
    base = jax.random.fold_in(key, 23)
    rows = []
    for step_index in range(STEPS):
        pieces = []
        for group_index in range(BATCH // BATCH_DEV):
            group_key = jax.random.fold_in(jax.random.fold_in(base, step_index), group_index)
            order = jax.random.permutation(group_key, POOL_DEV).astype(jnp.int32)
            pieces.append(order[:BATCH_DEV] + group_index * POOL_DEV)
        rows.append(jnp.concatenate(pieces))
    return jnp.stack(rows).astype(jnp.int32)


def steps_of(rng, extent, cuts, low, top_value):
    level = 1.0
    for position, shards_of in cuts:
        draws = jax.random.uniform(jax.random.fold_in(jax.random.fold_in(rng, 6), position), (shards_of,), jnp.float32, low / len(cuts), top_value / len(cuts))
        level = level * jnp.repeat(jnp.exp(draws), extent[position] // shards_of).reshape((-1,) + (1,) * (len(extent) - 1 - position))
    return level


def bell_draw(own_key, dims, scale, limit, cuts=(), kind=jnp.bfloat16):
    loudness = steps_of(own_key, dims, cuts, -0.22, 0.18) if cuts else 1.0
    drawn = jax.random.normal(own_key, dims, jnp.float32) * scale * loudness
    return jnp.minimum(jnp.maximum(drawn, -limit), limit).astype(kind)


def setup_inputs(seed: int = 0) -> dict:
    seeds = jax.random.split(jax.random.key(seed), 4)
    return {
        "pool_counts": draw_pool_counts(jax.random.fold_in(seeds[3], 71), 0),
        "cell_picks": draw_cell_picks(jax.random.fold_in(seeds[3], 71), 0),
        "loadings_init": bell_draw(seeds[2], (COMPS, GENES), GENES ** -0.5, 0.0390625, ((1, 8),), jnp.float32),
    }


step_rate = 1.0

def reference(pool_counts, cell_picks, loadings_init):
    loadings = loadings_init
    block_width = GENES // 8
    for step_index in range(STEPS):
        chosen = cell_picks[step_index]
        weights_low = loadings.astype(jnp.bfloat16)
        scores = jnp.zeros((COMPS, BATCH), jnp.float32)
        batch_means = []
        for block_index in range(8):
            lowest = block_index * block_width
            gathered = jnp.take(pool_counts[lowest:lowest + block_width], chosen, axis=1)
            means_part = lax.optimization_barrier(jnp.sum(gathered.astype(jnp.float32), axis=1)) / BATCH
            weight_part = weights_low[:, lowest:lowest + block_width]
            scores = scores + jnp.dot(weight_part.astype(jnp.float32), gathered.astype(jnp.float32), preferred_element_type=jnp.float32)
            shift = jnp.dot(weight_part.astype(jnp.float32), means_part, precision=lax.Precision.HIGHEST)
            scores = scores - shift[:, None]
            batch_means.append(means_part)
        scores_low = scores.astype(jnp.bfloat16)
        row_totals = lax.optimization_barrier(jnp.sum(scores_low.astype(jnp.float32), axis=1))
        updates = []
        for block_index in range(8):
            lowest = block_index * block_width
            gathered = jnp.take(pool_counts[lowest:lowest + block_width], chosen, axis=1)
            raw_update = lax.dot_general(scores_low.astype(jnp.float32), gathered.astype(jnp.float32), (((1,), (1,)), ((), ())), preferred_element_type=jnp.float32)
            updates.append((raw_update - row_totals[:, None] * batch_means[block_index][None, :]) / BATCH)
        update = jnp.concatenate(updates, axis=1)
        stepped = loadings + step_rate * update
        gram_matrix = jnp.dot(stepped, stepped.T, precision=lax.Precision.HIGHEST)
        factor = jnp.linalg.cholesky(gram_matrix)
        loadings = lax.linalg.triangular_solve(factor, stepped, left_side=True, lower=True)
    return loadings * math.sqrt(GENES)
```

```python
import functools
import math

import jax
import jax.numpy as jnp
from jax import lax
from jax.experimental import pallas as pl
from jax.experimental.pallas import tpu as pltpu
from jax.sharding import PartitionSpec as P

STEPS = 7
MESH = pl.DeviceIdType.MESH

step_rate = 1.0


def transposed_product(left, right):
    return lax.dot_general(
        left, right, (((1,), (1,)), ((), ())), preferred_element_type=jnp.float32
    )


def sum_kernel(axis, n, arrays, *refs):
    inputs, outputs = refs[:arrays], refs[arrays:2 * arrays]
    scratch = refs[2 * arrays:]
    landed, reduced, whole = (scratch[i * arrays:(i + 1) * arrays] for i in range(3))
    sends, arrivals, sends_back, arrivals_back = scratch[3 * arrays:]
    me = lax.axis_index(axis)
    barrier = pltpu.get_barrier_semaphore()
    peers = [lax.rem(me + k, n) for k in range(n)]
    for k in range(1, n):
        pl.semaphore_signal(barrier, inc=1, device_id={axis: peers[k]}, device_id_type=MESH)
    pl.semaphore_wait(barrier, n - 1)
    copies = []
    for a in range(arrays):
        for k in range(1, n):
            copy = pltpu.make_async_remote_copy(
                src_ref=inputs[a].at[peers[k]],
                dst_ref=landed[a].at[k - 1],
                send_sem=sends.at[a, k - 1],
                recv_sem=arrivals.at[a, k - 1],
                device_id={axis: peers[k]},
                device_id_type=MESH,
            )
            copy.start()
            copies.append(copy)
    for copy in copies:
        copy.wait_recv()
    backs = []
    for a in range(arrays):
        total = inputs[a][me].astype(jnp.float32)
        for k in range(1, n):
            total = total + landed[a][k - 1].astype(jnp.float32)
        reduced[a][...] = total.astype(reduced[a].dtype)
        for k in range(1, n):
            copy = pltpu.make_async_remote_copy(
                src_ref=reduced[a],
                dst_ref=whole[a].at[me],
                send_sem=sends_back.at[a, k - 1],
                recv_sem=arrivals_back.at[a, k - 1],
                device_id={axis: peers[k]},
                device_id_type=MESH,
            )
            copy.start()
            backs.append(copy)
        outputs[a][me] = reduced[a][...]
    for copy in copies:
        copy.wait_send()
    for copy in backs:
        copy.wait()
    for a in range(arrays):
        for k in range(1, n):
            outputs[a][peers[k]] = whole[a][peers[k]]


def sum_over(axis, n, collective_id, *arrays):
    cut = [a.reshape(n, a.shape[0] // n, a.shape[1]) for a in arrays]
    count = len(cut)
    scratch = [pltpu.VMEM((n - 1,) + a.shape[1:], a.dtype) for a in cut]
    scratch += [pltpu.VMEM(a.shape[1:], a.dtype) for a in cut]
    scratch += [pltpu.VMEM(a.shape, a.dtype) for a in cut]
    scratch += [pltpu.SemaphoreType.DMA((count, n - 1))] * 4
    outs = pl.pallas_call(
        functools.partial(sum_kernel, axis, n, count),
        out_shape=[jax.ShapeDtypeStruct(a.shape, a.dtype) for a in cut],
        in_specs=[pl.BlockSpec(memory_space=pltpu.VMEM)] * count,
        out_specs=[pl.BlockSpec(memory_space=pltpu.VMEM)] * count,
        scratch_shapes=scratch,
        compiler_params=pltpu.CompilerParams(
            collective_id=collective_id, has_side_effects=True
        ),
        name=f"sum_{axis}_{collective_id}",
    )(*cut)
    return [o.reshape(a.shape) for o, a in zip(outs, arrays)]


def inverse_factor(gram):
    size = gram.shape[0]
    rows = lax.broadcasted_iota(jnp.int32, (size, size), 0)
    columns = lax.broadcasted_iota(jnp.int32, (size, size), 1)
    left = gram
    right = jnp.where(rows == columns, 1.0, 0.0).astype(jnp.float32)
    for k in range(size):
        scale = 1.0 / jnp.sqrt(left[k:k + 1, k:k + 1])
        column = jnp.where(rows[:, :1] > k, left[:, k:k + 1] * scale, 0.0)
        left_row = left[k:k + 1, :] * scale
        right_row = right[k:k + 1, :] * scale
        left = left - column * left_row
        right = jnp.where(rows == k, right_row, right - column * right_row)
    return right


def exact_product(left, right):
    return jnp.dot(
        left, right, precision=lax.Precision.HIGHEST, preferred_element_type=jnp.float32
    )


def normalise_kernel(gram_ref, stepped_ref, *refs):
    inverse = inverse_factor(gram_ref[...])
    if len(refs) == 1:
        refs[0][...] = exact_product(inverse, stepped_ref[...])
        return
    raw_ref, loadings_ref, scores_ref = refs
    scores_ref[...] = exact_product(inverse, raw_ref[...].astype(jnp.float32)).astype(
        scores_ref.dtype
    )
    loadings_ref[...] = exact_product(inverse, stepped_ref[...])


def normalise(gram, stepped, raw=None):
    shapes = [jax.ShapeDtypeStruct(stepped.shape, jnp.float32)]
    operands = [gram, stepped]
    if raw is not None:
        shapes.append(jax.ShapeDtypeStruct(raw.shape, jnp.bfloat16))
        operands.append(raw)
    return pl.pallas_call(
        normalise_kernel,
        out_shape=shapes,
        in_specs=[pl.BlockSpec(memory_space=pltpu.VMEM)] * len(operands),
        out_specs=[pl.BlockSpec(memory_space=pltpu.VMEM)] * len(shapes),
        name="normalise",
    )(*operands)


def shards(genes, cells, pool_counts, cell_picks, loadings_init):
    stepped = loadings_init
    local_pool = pool_counts.shape[1]
    group = lax.axis_index("cell")
    batch_total = cell_picks.shape[1] * cells
    gene_total = stepped.shape[1] * genes
    tiles = [
        jnp.take(pool_counts, cell_picks[s] - group * local_pool, axis=1, mode="clip")
        for s in range(STEPS)
    ]
    sums = [jnp.sum(tile, axis=1, dtype=jnp.float32) for tile in tiles]
    padded = -(-STEPS // cells) * cells
    sums += [jnp.zeros_like(sums[0])] * (padded - STEPS)
    (totals,) = sum_over("cell", cells, 1, jnp.stack(sums))
    means = totals / batch_total
    for s in range(STEPS):
        mean = means[s]
        low = stepped.astype(jnp.bfloat16)
        product = jnp.dot(low, tiles[s], preferred_element_type=jnp.float32)
        shift = jnp.dot(low.astype(jnp.float32), mean, precision=lax.Precision.HIGHEST)
        part = (product - shift[:, None]).astype(jnp.bfloat16)
        if s == 0:
            (scores_low,) = sum_over("gene", genes, 2, part)
            loadings = stepped
        else:
            gram_part = jnp.dot(stepped, stepped.T, precision=lax.Precision.HIGHEST)
            raw, gram = sum_over("gene", genes, 3, part, gram_part)
            loadings, scores_low = normalise(gram, stepped, raw)
        raw_update = transposed_product(scores_low, tiles[s])
        row_totals = jnp.sum(scores_low, axis=1, dtype=jnp.float32)
        local = (raw_update - row_totals[:, None] * mean[None, :]) / batch_total
        (update,) = sum_over("cell", cells, 4, local.astype(jnp.bfloat16))
        stepped = loadings + step_rate * update.astype(jnp.float32)
    gram_part = jnp.dot(stepped, stepped.T, precision=lax.Precision.HIGHEST)
    (gram,) = sum_over("gene", genes, 5, gram_part)
    (loadings,) = normalise(gram, stepped)
    return loadings * math.sqrt(gene_total)


def solution(mesh):
    placed = (P("gene", "cell"), P(None, "cell"), P(None, "gene"))
    return jax.shard_map(
        functools.partial(shards, mesh.shape["gene"], mesh.shape["cell"]),
        mesh=mesh, in_specs=placed, out_specs=P(None, "gene"), check_vma=False,
    )
```

```python
import functools
import math

import jax
import jax.numpy as jnp
from jax import lax
from jax.experimental import pallas as pl
from jax.experimental.pallas import tpu as pltpu
from jax.sharding import PartitionSpec as P

STEPS = 7
MESH = pl.DeviceIdType.MESH

step_rate = 1.0


def transposed_product(left, right):
    return lax.dot_general(
        left, right, (((1,), (1,)), ((), ())), preferred_element_type=jnp.float32
    )


def sum_kernel(axis, n, arrays, gather, *refs):
    inputs = refs[:arrays]
    refs = refs[arrays:]
    if gather:
        pool_ref, picks_ref = refs[:2]
        refs = refs[2:]
    outputs = refs[:arrays]
    refs = refs[arrays:]
    if gather:
        tile_ref = refs[0]
        refs = refs[1:]
    landed, reduced, whole = (refs[i * arrays:(i + 1) * arrays] for i in range(3))
    sends, arrivals, sends_back, arrivals_back = refs[3 * arrays:3 * arrays + 4]
    me = lax.axis_index(axis)
    barrier = pltpu.get_barrier_semaphore()
    peers = [lax.rem(me + k, n) for k in range(n)]
    for k in range(1, n):
        pl.semaphore_signal(barrier, inc=1, device_id={axis: peers[k]}, device_id_type=MESH)
    blocks = 0
    if gather:
        held, hot, loaded = refs[3 * arrays + 4:]
        start, block, blocks = gather
        loads = []
        for b in range(blocks):
            load = pltpu.make_async_copy(
                pool_ref.at[pl.ds(start + b * block, block)],
                held.at[pl.ds(b * block, block)],
                loaded.at[b],
            )
            load.start()
            loads.append(load)

    def select_columns(b):
        loads[b].wait()
        rows = pl.ds(b * block, block)
        width = min(512, hot.shape[1])

        def piece(j, carry):
            columns = pl.ds(pl.multiple_of(j * width, width), width)
            tile_ref[rows, columns] = jnp.dot(
                held[rows, :], hot[:, columns], preferred_element_type=jnp.float32
            ).astype(tile_ref.dtype)
            return carry

        lax.fori_loop(0, hot.shape[1] // width, piece, 0)

    pl.semaphore_wait(barrier, n - 1)
    copies = []
    for a in range(arrays):
        for k in range(1, n):
            copy = pltpu.make_async_remote_copy(
                src_ref=inputs[a].at[peers[k]],
                dst_ref=landed[a].at[k - 1],
                send_sem=sends.at[a, k - 1],
                recv_sem=arrivals.at[a, k - 1],
                device_id={axis: peers[k]},
                device_id_type=MESH,
            )
            copy.start()
            copies.append(copy)
    if gather:
        depth = 256

        def mark(i, carry):
            ids = lax.broadcasted_iota(jnp.int32, (depth, hot.shape[1]), 0) + i * depth
            hot[pl.ds(pl.multiple_of(i * depth, depth), depth), :] = jnp.where(
                ids == picks_ref[...], 1.0, 0.0
            ).astype(hot.dtype)
            return carry

        lax.fori_loop(0, hot.shape[0] // depth, mark, 0)
    early = blocks // 2
    for b in range(early):
        select_columns(b)
    for copy in copies:
        copy.wait_recv()
    backs = []
    for a in range(arrays):
        total = inputs[a][me].astype(jnp.float32)
        for k in range(1, n):
            total = total + landed[a][k - 1].astype(jnp.float32)
        reduced[a][...] = total.astype(reduced[a].dtype)
        for k in range(1, n):
            copy = pltpu.make_async_remote_copy(
                src_ref=reduced[a],
                dst_ref=whole[a].at[me],
                send_sem=sends_back.at[a, k - 1],
                recv_sem=arrivals_back.at[a, k - 1],
                device_id={axis: peers[k]},
                device_id_type=MESH,
            )
            copy.start()
            backs.append(copy)
        outputs[a][me] = reduced[a][...]
    for b in range(early, blocks):
        select_columns(b)
    for copy in copies:
        copy.wait_send()
    for copy in backs:
        copy.wait()
    for a in range(arrays):
        for k in range(1, n):
            outputs[a][peers[k]] = whole[a][peers[k]]


def sum_over(axis, n, collective_id, arrays, gather=None):
    cut = [a.reshape(n, a.shape[0] // n, a.shape[1]) for a in arrays]
    count = len(cut)
    vmem = pl.BlockSpec(memory_space=pltpu.VMEM)
    operands, in_specs = list(cut), [vmem] * count
    shapes = [jax.ShapeDtypeStruct(a.shape, a.dtype) for a in cut]
    scratch = [pltpu.VMEM((n - 1,) + a.shape[1:], a.dtype) for a in cut]
    scratch += [pltpu.VMEM(a.shape[1:], a.dtype) for a in cut]
    scratch += [pltpu.VMEM(a.shape, a.dtype) for a in cut]
    scratch += [pltpu.SemaphoreType.DMA((count, n - 1))] * 4
    plan = None
    if gather is not None:
        pool, picks, start, rows = gather
        block = 256 if rows % 256 == 0 else rows
        plan = (start, block, rows // block)
        operands += [pool, picks[None, :]]
        in_specs += [pl.BlockSpec(memory_space=pl.ANY), vmem]
        shapes.append(jax.ShapeDtypeStruct((rows, picks.shape[0]), pool.dtype))
        scratch += [
            pltpu.VMEM((rows, pool.shape[1]), pool.dtype),
            pltpu.VMEM((pool.shape[1], picks.shape[0]), pool.dtype),
            pltpu.SemaphoreType.DMA((rows // block,)),
        ]
    outs = pl.pallas_call(
        functools.partial(sum_kernel, axis, n, count, plan),
        out_shape=shapes,
        in_specs=in_specs,
        out_specs=[vmem] * len(shapes),
        scratch_shapes=scratch,
        compiler_params=pltpu.CompilerParams(
            collective_id=collective_id, has_side_effects=True,
            vmem_limit_bytes=48 * 1024 * 1024,
        ),
        name=f"sum_{axis}_{collective_id}",
    )(*operands)
    return [o.reshape(a.shape) for o, a in zip(outs, arrays)] + list(outs[count:])


def inverse_factor(gram):
    size = gram.shape[0]
    rows = lax.broadcasted_iota(jnp.int32, (size, size), 0)
    columns = lax.broadcasted_iota(jnp.int32, (size, size), 1)
    left = gram
    right = jnp.where(rows == columns, 1.0, 0.0).astype(jnp.float32)
    for k in range(size):
        scale = 1.0 / jnp.sqrt(left[k:k + 1, k:k + 1])
        column = jnp.where(rows[:, :1] > k, left[:, k:k + 1] * scale, 0.0)
        left_row = left[k:k + 1, :] * scale
        right_row = right[k:k + 1, :] * scale
        left = left - column * left_row
        right = jnp.where(rows == k, right_row, right - column * right_row)
    return right


def exact_product(left, right):
    return jnp.dot(
        left, right, precision=lax.Precision.HIGHEST, preferred_element_type=jnp.float32
    )


def normalise_kernel(gram_ref, stepped_ref, *refs):
    inverse = inverse_factor(gram_ref[...])
    if len(refs) == 1:
        refs[0][...] = exact_product(inverse, stepped_ref[...])
        return
    raw_ref, loadings_ref, scores_ref = refs
    scores_ref[...] = exact_product(inverse, raw_ref[...].astype(jnp.float32)).astype(
        scores_ref.dtype
    )
    loadings_ref[...] = exact_product(inverse, stepped_ref[...])


def normalise(gram, stepped, raw=None):
    shapes = [jax.ShapeDtypeStruct(stepped.shape, jnp.float32)]
    operands = [gram, stepped]
    if raw is not None:
        shapes.append(jax.ShapeDtypeStruct(raw.shape, jnp.bfloat16))
        operands.append(raw)
    return pl.pallas_call(
        normalise_kernel,
        out_shape=shapes,
        in_specs=[pl.BlockSpec(memory_space=pltpu.VMEM)] * len(operands),
        out_specs=[pl.BlockSpec(memory_space=pltpu.VMEM)] * len(shapes),
        name="normalise",
    )(*operands)


def select(pool, picks, start):
    ids = jnp.arange(pool.shape[1], dtype=jnp.int32)
    hot = (ids[:, None] == picks[None, :]).astype(pool.dtype)
    return jnp.dot(pool[start:], hot, preferred_element_type=jnp.float32).astype(pool.dtype)


def shards(genes, cells, pool_counts, cell_picks, loadings_init):
    stepped = loadings_init
    local_pool = pool_counts.shape[1]
    group = lax.axis_index("cell")
    batch_total = cell_picks.shape[1] * cells
    local_genes = stepped.shape[1]
    gene_total = local_genes * genes
    picks = cell_picks - group * local_pool
    ids = jnp.arange(local_pool, dtype=jnp.int32)
    chosen = jnp.any(picks[:, :, None] == ids[None, None, :], axis=1).astype(jnp.bfloat16)
    sums = transposed_product(chosen, pool_counts)
    sums = jnp.pad(sums, ((0, -STEPS % cells), (0, 0)))
    split = local_genes // 2
    totals, upper = sum_over("cell", cells, 1, [sums], (pool_counts, picks[0], 0, split))
    lower = select(pool_counts, picks[0], split)
    means = totals / batch_total
    for s in range(STEPS):
        last = s == STEPS - 1
        mean = means[s]
        low = stepped.astype(jnp.bfloat16)
        product = jnp.dot(low[:, :split], upper, preferred_element_type=jnp.float32)
        product += jnp.dot(low[:, split:], lower, preferred_element_type=jnp.float32)
        shift = jnp.dot(low.astype(jnp.float32), mean, precision=lax.Precision.HIGHEST)
        part = (product - shift[:, None]).astype(jnp.bfloat16)
        ahead = None if last else (pool_counts, picks[s + 1], 0, split)
        if s == 0:
            scores_low, *next_upper = sum_over("gene", genes, 2, [part], ahead)
            loadings = stepped
        else:
            gram_part = jnp.dot(stepped, stepped.T, precision=lax.Precision.HIGHEST)
            raw, gram, *next_upper = sum_over(
                "gene", genes, 6 if last else 3, [part, gram_part], ahead
            )
            loadings, scores_low = normalise(gram, stepped, raw)
        raw_update = jnp.concatenate(
            [transposed_product(scores_low, upper), transposed_product(scores_low, lower)], axis=1
        )
        row_totals = jnp.sum(scores_low, axis=1, dtype=jnp.float32)
        local = (raw_update - row_totals[:, None] * mean[None, :]) / batch_total
        ahead = None if last else (pool_counts, picks[s + 1], split, local_genes - split)
        update, *next_lower = sum_over(
            "cell", cells, 7 if last else 4, [local.astype(jnp.bfloat16)], ahead
        )
        if not last:
            upper, lower = next_upper[0], next_lower[0]
        stepped = loadings + step_rate * update.astype(jnp.float32)
    gram_part = jnp.dot(stepped, stepped.T, precision=lax.Precision.HIGHEST)
    (gram,) = sum_over("gene", genes, 5, [gram_part])
    (loadings,) = normalise(gram, stepped)
    return loadings * math.sqrt(gene_total)


def solution(mesh):
    placed = (P("gene", "cell"), P(None, "cell"), P(None, "gene"))
    return jax.shard_map(
        functools.partial(shards, mesh.shape["gene"], mesh.shape["cell"]),
        mesh=mesh, in_specs=placed, out_specs=P(None, "gene"), check_vma=False,
    )
```
